32 devices in a mesh: tilt: 2 (over y), row: 8 (over z, x), col: 2 (over core).
Axes of the slice: x: 2, y: 2, z: 4, core: 2. Of those that a mesh axis runs over, the one named last changes fastest.
Arguments:
- object_field: float32 [2, 2048, 256], P(None, ('tilt', 'row'), 'col'), parts along dimension 1, may hold values from -4.2 to 4.2
- probe: float32 [8, 2, 128, 128], P('tilt'), parts along dimension 0, may hold values from -2.1 to 2.1
- patterns: float32 [16, 2, 2, 128, 128], P(('tilt', 'row'), 'col'), parts along dimension 0, may hold values from 0.1 to 3
- offsets: int32 [16, 2, 2, 2], P(('tilt', 'row'), 'col'), parts along dimension 0, may hold values from 0 to 256
- counts: int32 [16, 2], P(('tilt', 'row'), 'col'), parts along dimension 0, may hold values from 1 to 2, as said below
Outputs:
- object_out: float32 [2, 2048, 256], P(None, ('tilt', 'row'), 'col'), parts along dimension 1
- probe_out: float32 [8, 2, 128, 128], P('tilt'), parts along dimension 0
The draws below stay inside these ranges and needn't reach their ends.
There are 2 independent parts, one for each index of `tilt`. The reference program is written for one: setup_inputs(seed, part) draws one part's arguments, and reference() takes and returns one part's arrays. A program takes and returns all parts, laid end to end along the dimension named above; each array names one. Nothing has to cross between parts.
Inputs may be any that keep to these rules, and one draw needn't show every extreme that they name: Only the first counts[r, c] slots of a tile are live; some tile has all 2 live. `offsets`: A window lies inside its tile's frame of 384 pixels a side.
All inputs are finite; a program needn't handle non-finite values.
Results may differ from the reference program's by a relative error of at most 0.0003.
Values sent between devices are 32-bit elements; how exact they have to be, the bound alone decides.
A program may use at most 64 MiB of HBM per device.

```python
import math
import jax
import jax.numpy as jnp
from jax import lax

B = 128
H = 128
P_SIZE = 128
MODES = 4
POS = 2
ITERS = 1
TILE_ROWS = 8
TILE_COLS = 2
NY = 1024
NX = 256


def draw_counts(key, part):
    light_key = jax.random.fold_in(key, 101)
    busy_key = jax.random.fold_in(key, 202)
    chosen_key = jax.random.fold_in(key, 303)
    light_tiles = jax.random.randint(light_key, (TILE_ROWS, TILE_COLS), 1, max(POS // 2, 1) + 1)
    busy_tiles = jax.random.randint(busy_key, (TILE_ROWS, TILE_COLS), 0, 8) == 0
    filled = jnp.where(busy_tiles, POS, light_tiles).reshape(-1)
    chosen_tile = jax.random.randint(chosen_key, (), 0, TILE_ROWS * TILE_COLS)
    filled = filled.at[chosen_tile].set(POS)
    return filled.reshape(TILE_ROWS, TILE_COLS).astype(jnp.int32)


def plant(result, rng, least, top_value):
    shape = result.shape
    spot = [jax.random.randint(jax.random.fold_in(rng, axis), (), 0, shape[axis]) for axis in range(len(shape))]
    result = result.at[tuple(spot)].set(least)
    longest = shape.index(max(shape))
    spot[longest] = (spot[longest] + 1) % shape[longest]
    return result.at[tuple(spot)].set(top_value)


def steps_of(rng, shape, shards, least, top_value):
    def one(dim, blocks):
        draws = jax.random.uniform(jax.random.fold_in(jax.random.fold_in(rng, 6), dim), (blocks,), jnp.float32, least / len(shards), top_value / len(shards))
        return jnp.repeat(jnp.exp(draws), shape[dim] // blocks).reshape((-1,) + (1,) * (len(shape) - dim - 1))

    factor_of = one(*shards[0])
    for cut in shards[1:]:
        factor_of = factor_of * one(*cut)
    return factor_of


def scatter_about(key, dims, spread, most, cuts=(), kind=jnp.bfloat16):
    entries = spread * jax.random.normal(key, dims, jnp.float32)
    if cuts:
        entries = entries * steps_of(key, dims, cuts, -0.22, 0.18)
    return jnp.clip(entries, -most, most).astype(kind)


def setup_inputs(seed: int = 0, part: int = 0) -> dict:
    keys = jax.random.split(jax.random.key(seed), 6)
    part_keys = jax.random.split(jax.random.fold_in(keys[5], part), 6)
    object_field = scatter_about(part_keys[0], (2, NY, NX), 0.7, 4.2, ((1, 8), (2, 2)), jnp.float32)
    probe = scatter_about(part_keys[1], (MODES, 2, P_SIZE, P_SIZE), 0.35, 2.1, (), jnp.float32)
    patterns = jnp.clip(jnp.exp(math.log(3.0) - 3.4011974 * jax.random.uniform(part_keys[2], (TILE_ROWS, TILE_COLS, POS, P_SIZE, P_SIZE), jnp.float32) ** steps_of(part_keys[2], (TILE_ROWS, TILE_COLS, POS, P_SIZE, P_SIZE), ((0, 8), (1, 2)), -0.2, 0.2)), 0.1, 3.0)
    offsets = plant(jax.random.randint(part_keys[3], (TILE_ROWS, TILE_COLS, POS, 2), 0, B + 2 * H - P_SIZE + 1), jax.random.fold_in(part_keys[3], 1), 0, B + 2 * H - P_SIZE).astype(jnp.int32)
    counts = draw_counts(jax.random.fold_in(jax.random.fold_in(keys[5], part), 71), part)
    return dict(object_field=object_field, probe=probe, patterns=patterns, offsets=offsets, counts=counts)


object_rate = 1.0
probe_rate = 1.0
epsilon = 1e-06

def as_index(value):
    return jnp.asarray(value).astype(jnp.int32)

def dft_tables(length):
    counter = jnp.arange(length, dtype=jnp.int32)
    product = counter[:, None] * counter[None, :] % length
    angle = -2.0 * jnp.pi / length * product.astype(jnp.float32)
    norm = 1.0 / jnp.sqrt(jnp.float32(length))
    return (jnp.cos(angle) * norm, jnp.sin(angle) * norm)

def left_product(cos_table, sin_table, real_part, imag_part):
    hp = lax.Precision.HIGHEST
    real_out = jnp.einsum('ab,kbc->kac', cos_table, real_part, precision=hp) - jnp.einsum('ab,kbc->kac', sin_table, imag_part, precision=hp)
    imag_out = jnp.einsum('ab,kbc->kac', cos_table, imag_part, precision=hp) + jnp.einsum('ab,kbc->kac', sin_table, real_part, precision=hp)
    return (real_out, imag_out)

def right_product(real_part, imag_part, cos_table, sin_table):
    hp = lax.Precision.HIGHEST
    real_out = jnp.einsum('kab,bc->kac', real_part, cos_table, precision=hp) - jnp.einsum('kab,bc->kac', imag_part, sin_table, precision=hp)
    imag_out = jnp.einsum('kab,bc->kac', real_part, sin_table, precision=hp) + jnp.einsum('kab,bc->kac', imag_part, cos_table, precision=hp)
    return (real_out, imag_out)

def transform(real_part, imag_part, cos_table, sin_table):
    middle_re, middle_im = left_product(cos_table, sin_table, real_part, imag_part)
    return right_product(middle_re, middle_im, cos_table, sin_table)

def slot_terms(window, probe, pattern, cos_table, sin_table):
    window_re, window_im = (window[0], window[1])
    probe_re, probe_im = (probe[:, 0], probe[:, 1])
    exit_re = probe_re * window_re - probe_im * window_im
    exit_im = probe_re * window_im + probe_im * window_re
    far_re, far_im = transform(exit_re, exit_im, cos_table, sin_table)
    intensity = lax.optimization_barrier(jnp.sum(far_re * far_re + far_im * far_im, axis=0))
    misfit = intensity - pattern
    back_re, back_im = transform(misfit * far_re, misfit * far_im, cos_table, -sin_table)
    grad_re = lax.optimization_barrier(jnp.sum(probe_re * back_re + probe_im * back_im, axis=0))
    grad_im = lax.optimization_barrier(jnp.sum(probe_re * back_im - probe_im * back_re, axis=0))
    term_re = window_re * back_re + window_im * back_im
    term_im = window_re * back_im - window_im * back_re
    return (jnp.stack([grad_re, grad_im]), jnp.stack([term_re, term_im], axis=1))

def reference(object_field, probe, patterns, offsets, counts):
    cos_table, sin_table = dft_tables(P_SIZE)
    frame_size = B + 2 * H
    for iteration in range(ITERS):
        padded = jnp.pad(object_field, ((0, 0), (H, H), (H, H)))

        def tile_step(carry, tile_index):
            gradient, probe_grad = carry
            tile_row = as_index(tile_index // TILE_COLS)
            tile_col = as_index(tile_index % TILE_COLS)
            frame = lax.dynamic_slice(padded, (as_index(0), tile_row * B, tile_col * B), (2, frame_size, frame_size))

            def slot_step(slot_index, inner):
                local_grad, probe_acc = inner
                slot_index = as_index(slot_index)
                corner_y = as_index(offsets[tile_row, tile_col, slot_index, 0])
                corner_x = as_index(offsets[tile_row, tile_col, slot_index, 1])
                window = lax.dynamic_slice(frame, (as_index(0), corner_y, corner_x), (2, P_SIZE, P_SIZE))
                window_grad, probe_term = slot_terms(window, probe, patterns[tile_row, tile_col, slot_index], cos_table, sin_table)
                live = (slot_index < counts[tile_row, tile_col]).astype(jnp.float32)
                region = lax.dynamic_slice(local_grad, (as_index(0), corner_y, corner_x), (2, P_SIZE, P_SIZE)) + live * window_grad
                local_grad = lax.dynamic_update_slice(local_grad, region, (as_index(0), corner_y, corner_x))
                return (local_grad, probe_acc + live * probe_term)
            local_grad = jnp.zeros((2, frame_size, frame_size), jnp.float32)
            local_grad, probe_grad = lax.fori_loop(0, POS, slot_step, (local_grad, probe_grad))
            start = (as_index(0), tile_row * B, tile_col * B)
            region = lax.dynamic_slice(gradient, start, (2, frame_size, frame_size)) + local_grad
            gradient = lax.dynamic_update_slice(gradient, region, start)
            return ((gradient, probe_grad), None)
        start_carry = (jnp.zeros_like(padded), jnp.zeros_like(probe))
        (gradient, probe_grad), unused = lax.scan(tile_step, start_carry, jnp.arange(TILE_ROWS * TILE_COLS, dtype=jnp.int32))
        object_grad = gradient[:, H:H + NY, H:H + NX]
        weight = jnp.max(lax.optimization_barrier(jnp.sum(probe[:, 0] * probe[:, 0] + probe[:, 1] * probe[:, 1], axis=0))) + epsilon
        object_field = object_field - object_rate * object_grad / weight
        probe = probe - probe_rate * probe_grad / (TILE_ROWS * TILE_COLS)
    return (object_field, probe)
```

```python
import functools

import jax
import jax.numpy as jnp
import numpy as np
from jax import lax
from jax.experimental import pallas as pl
from jax.experimental.pallas import tpu as pltpu
from jax.sharding import PartitionSpec as P

MESH = pl.DeviceIdType.MESH
F32 = jnp.float32
BF16 = jnp.bfloat16

object_rate = 1.0
probe_rate = 1.0
epsilon = 1e-06


def split_table(table):
    high = table.astype(jnp.bfloat16)
    low = (table - high.astype(np.float64)).astype(jnp.bfloat16)
    return high, low


def dft_tables(length):
    counter = np.arange(length)
    product = counter[:, None] * counter[None, :] % length
    angle = -2.0 * np.pi / length * product
    c, s = np.cos(angle) / np.sqrt(length), np.sin(angle) / np.sqrt(length)
    right = np.block([[c, s], [-s, c]])
    left = right.T
    return np.stack([*split_table(right), *split_table(left)])


def split(x):
    high = x.astype(BF16)
    return high, (x - high.astype(F32)).astype(BF16)


def each_peer(total, step):
    if total <= 16:
        for hop in range(1, total):
            step(hop)
    else:
        lax.fori_loop(1, total, lambda hop, carry: (step(hop), carry)[1], 0)


def dot(a, b):
    return jnp.dot(a, b, preferred_element_type=F32)


def kernel(
    rows, modes, slots, width, owners,
    off_ref, cnt_ref, obj_ref, probe_ref, pat_ref, tab_ref,
    obj_out, probe_out,
    frame, xh, xl, yh, yl, far, vh, vl, win, gacc,
    gown, gpar, grecv, gedge, term, tpart, acc, pieces, red, red_other,
    h_send, h_recv, g_send, g_recv, e_send, e_recv, t_send, t_recv,
    rs_send, rs_recv, ag_send, ag_recv, o_send, o_recv,
):
    me = lax.axis_index("row")
    col = lax.axis_index("col")
    n = width
    tiles = rows * 2
    mate = {"col": 1 - col}
    up = {"row": me - 1}
    down = {"row": me + 1}
    has_up, has_down = me > 0, me < rows - 1
    chunk = 2 * n // owners

    barrier = pltpu.get_barrier_semaphore()
    pl.semaphore_signal(barrier, inc=1, device_id=mate, device_id_type=MESH)

    def greet(hop):
        other = lax.rem(me + hop, rows)
        pl.semaphore_signal(barrier, inc=1, device_id={"row": other}, device_id_type=MESH)

    each_peer(rows, greet)
    pl.semaphore_wait(barrier, rows)

    def remote(src, dst, send, recv, to):
        return pltpu.make_async_remote_copy(
            src_ref=src, dst_ref=dst, send_sem=send, recv_sem=recv, device_id=to, device_id_type=MESH
        )

    seen = 2 * col
    mine = 2 - 2 * col
    to_mate = remote(obj_ref, frame.at[1, seen], h_send.at[0], h_recv.at[0], mate)
    to_up = remote(obj_ref, frame.at[2, 1], h_send.at[1], h_recv.at[2], up)
    to_down = remote(obj_ref, frame.at[0, 1], h_send.at[2], h_recv.at[1], down)
    relay_up = remote(frame.at[0, 1], frame.at[0, seen], h_send.at[3], h_recv.at[3], mate)
    relay_down = remote(frame.at[2, 1], frame.at[2, seen], h_send.at[4], h_recv.at[4], mate)
    pl.when(has_up)(to_up.start)
    pl.when(has_down)(to_down.start)
    to_mate.start()

    zero = jnp.zeros((2, n, n), F32)
    frame[1, 1] = obj_ref[...]
    for j in range(3):
        frame[j, seen] = zero

    @pl.when(me == 0)
    def _():
        frame[0, 1] = zero
        frame[0, mine] = zero

    @pl.when(me == rows - 1)
    def _():
        frame[2, 1] = zero
        frame[2, mine] = zero

    power = jnp.zeros((n, n), F32)
    for k in range(modes):
        power = power + (probe_ref[k, 0] * probe_ref[k, 0] + probe_ref[k, 1] * probe_ref[k, 1])
    weight = jnp.max(power) + epsilon

    @pl.when(has_up)
    def _():
        to_down.wait_recv()
        relay_up.start()

    @pl.when(has_down)
    def _():
        to_up.wait_recv()
        relay_down.start()

    to_mate.wait_recv()
    pl.when(has_up)(relay_up.wait_recv)
    pl.when(has_down)(relay_down.wait_recv)

    r_hi, r_lo, l_hi, l_lo = (tab_ref.at[t] for t in range(4))
    row_id = lax.broadcasted_iota(jnp.int32, (n, n), 0)
    lane_id = lax.broadcasted_iota(jnp.int32, (n, n), 1)

    def place(s):
        oy, ox = off_ref[0, 0, s, 0], off_ref[0, 0, s, 1]
        by, bx = oy // n, ox // n
        return by, bx, oy - by * n, ox - bx * n

    for s in range(slots):
        by, bx, sy, sx = place(s)
        by2, bx2 = jnp.minimum(by + 1, 2), jnp.minimum(bx + 1, 2)
        for q in range(2):
            upper = jnp.where(lane_id >= sx, frame[by, bx, q], frame[by, bx2, q])
            lower = jnp.where(lane_id >= sx, frame[by2, bx, q], frame[by2, bx2, q])
            packed = jnp.where(row_id >= sy, upper, lower)
            packed = pltpu.roll(packed, lax.rem(n - sy, n), 0)
            win[s, q] = pltpu.roll(packed, lax.rem(n - sx, n), 1)
        for k in range(modes):
            wr, wi = win[s, 0], win[s, 1]
            pr, pi = probe_ref[k, 0], probe_ref[k, 1]
            for q, part in enumerate((pr * wr - pi * wi, pr * wi + pi * wr)):
                hi, lo = split(part)
                xh[s, k * n : (k + 1) * n, q * n : (q + 1) * n] = hi
                xl[s, k * n : (k + 1) * n, q * n : (q + 1) * n] = lo
        for k in range(modes):
            a_hi, a_lo = xh[s, k * n : (k + 1) * n, :], xl[s, k * n : (k + 1) * n, :]
            y = dot(a_hi, r_hi[...]) + dot(a_lo, r_hi[...]) + dot(a_hi, r_lo[...])
            for q in range(2):
                hi, lo = split(y[:, q * n : (q + 1) * n])
                yh[s, q * n : (q + 1) * n, k * n : (k + 1) * n] = hi
                yl[s, q * n : (q + 1) * n, k * n : (k + 1) * n] = lo
        for p in range(modes // 2):
            cols = slice(2 * p * n, 2 * (p + 1) * n)
            b_hi, b_lo = yh[s, :, cols], yl[s, :, cols]
            far[s, :, cols] = dot(l_hi[...], b_hi) + dot(l_lo[...], b_hi) + dot(l_hi[...], b_lo)
        level = jnp.zeros((n, n), F32)
        for k in range(modes):
            cols = slice(k * n, (k + 1) * n)
            level = level + far[s, :n, cols] * far[s, :n, cols] + far[s, n:, cols] * far[s, n:, cols]
        live = (s < cnt_ref[0, 0]).astype(F32)
        misfit = live * (level - pat_ref[0, 0, s])
        for k in range(modes):
            for q in range(2):
                spot = (s, slice(q * n, (q + 1) * n), slice(k * n, (k + 1) * n))
                hi, lo = split(misfit * far[spot])
                yh[spot] = hi
                yl[spot] = lo

    def to_partner(p):
        return remote(term.at[2 * p + 1 - col], tpart.at[p], t_send.at[p], t_recv.at[p], mate)

    for p in range(modes // 2):
        cols = slice(2 * p * n, 2 * (p + 1) * n)
        for s in range(slots):
            b_hi, b_lo = yh[s, :, cols], yl[s, :, cols]
            v = dot(r_hi[...], b_hi) + dot(r_lo[...], b_hi) + dot(r_hi[...], b_lo)
            for m in range(2):
                for q in range(2):
                    hi, lo = split(v[q * n : (q + 1) * n, m * n : (m + 1) * n])
                    vh[s, m * n : (m + 1) * n, q * n : (q + 1) * n] = hi
                    vl[s, m * n : (m + 1) * n, q * n : (q + 1) * n] = lo
            for m in range(2):
                k = 2 * p + m
                a_hi, a_lo = vh[s, m * n : (m + 1) * n, :], vl[s, m * n : (m + 1) * n, :]
                back = dot(a_hi, l_hi[...]) + dot(a_lo, l_hi[...]) + dot(a_hi, l_lo[...])
                br, bi = back[:, :n], back[:, n:]
                pr, pi = probe_ref[k, 0], probe_ref[k, 1]
                gr, gi = pr * br + pi * bi, pr * bi - pi * br
                wr, wi = win[s, 0], win[s, 1]
                tr, ti = wr * br + wi * bi, wr * bi - wi * br
                if k == 0:
                    gacc[s, 0], gacc[s, 1] = gr, gi
                else:
                    gacc[s, 0], gacc[s, 1] = gacc[s, 0] + gr, gacc[s, 1] + gi
                if s == 0:
                    term[k, 0], term[k, 1] = tr, ti
                else:
                    term[k, 0], term[k, 1] = term[k, 0] + tr, term[k, 1] + ti
        to_partner(p).start()

    for q in range(2):
        own = [jnp.zeros((n, n), F32)] * 3
        par = [jnp.zeros((n, n), F32)] * 3
        for s in range(slots):
            by, bx, sy, sx = place(s)
            g = pltpu.roll(pltpu.roll(gacc[s, q], sy, 0), sx, 1)
            low_x, low_y = (lane_id >= sx).astype(F32), (row_id >= sy).astype(F32)

            def side(block, at, low):
                return (block == at).astype(F32) * low + (block == at + 1).astype(F32) * (1.0 - low)

            g_own, g_par = g * side(1, bx, low_x), g * side(mine, bx, low_x)
            for j in range(3):
                mask = side(j, by, low_y)
                own[j] = own[j] + g_own * mask
                par[j] = par[j] + g_par * mask
        for j in range(3):
            gown[j, q] = own[j]
            gpar[j, q] = par[j]
    across = remote(gpar, grecv, g_send.at[0], g_recv.at[0], mate)
    across.start()

    def row_slice(ref, p, owner):
        return ref.at[p, pl.ds(pl.multiple_of(owner * chunk, 8), chunk)]

    def scatter(p, hop):
        to = lax.rem(me + hop, rows)
        src = lax.rem(me + rows - hop, rows)
        return (
            to,
            remote(row_slice(acc, p, to), pieces.at[p, hop], rs_send.at[p, hop], rs_recv.at[p, hop], {"row": to}),
        )

    def start_scatter(p):
        to_partner(p).wait()
        for q in range(2):
            acc[p, q * n : (q + 1) * n] = term[2 * p + col, q] + tpart[p, q]

        def step(hop):
            to, copy = scatter(p, hop)
            pl.when(to < owners)(copy.start)

        each_peer(rows, step)

    start_scatter(0)

    across.wait()
    for j in range(3):
        gown[j] = gown[j] + grecv[j]
    edge_up = remote(gown.at[0], gedge.at[1], e_send.at[0], e_recv.at[1], up)
    edge_down = remote(gown.at[2], gedge.at[0], e_send.at[1], e_recv.at[0], down)
    pl.when(has_up)(edge_up.start)
    pl.when(has_down)(edge_down.start)

    for p in range(1, modes // 2):
        start_scatter(p)

    def gather(p, hop):
        to = lax.rem(me + hop, rows)
        here = row_slice(red, p, me)
        return remote(here, here, ag_send.at[p, hop], ag_recv.at[p, hop], {"row": to})

    for p in range(modes // 2):

        @pl.when(me < owners)
        def _():
            red_chunk = row_slice(acc, p, me)[...]

            if rows <= 16:
                for hop in range(1, rows):
                    scatter(p, hop)[1].wait_recv()
                    red_chunk = red_chunk + pieces[p, hop]
            else:

                def add(hop, total):
                    scatter(p, hop)[1].wait_recv()
                    return total + pieces[p, hop]

                red_chunk = lax.fori_loop(1, rows, add, red_chunk)
            row_slice(red, p, me)[...] = red_chunk
            each_peer(rows, lambda hop: gather(p, hop).start())

    @pl.when(jnp.logical_not(has_up))
    def _():
        gedge[0] = zero

    @pl.when(jnp.logical_not(has_down))
    def _():
        gedge[1] = zero

    pl.when(has_up)(edge_down.wait_recv)
    pl.when(has_down)(edge_up.wait_recv)
    for q in range(2):
        grad = gown[1, q] + gedge[0, q] + gedge[1, q]
        obj_out[q] = obj_ref[q] - object_rate * grad / weight

    def swap(p):
        return remote(red.at[p], red_other.at[p], o_send.at[p], o_recv.at[p], mate)

    for p in range(modes // 2):

        def step(hop):
            src = lax.rem(me + rows - hop, rows)
            pl.when(src < owners)(gather(p, hop).wait_recv)

        each_peer(rows, step)
        swap(p).start()
        k = 2 * p + col
        for q in range(2):
            probe_out[k, q] = probe_ref[k, q] - probe_rate * red[p, q * n : (q + 1) * n] / tiles
    for p in range(modes // 2):
        swap(p).wait()
        k = 2 * p + 1 - col
        for q in range(2):
            probe_out[k, q] = probe_ref[k, q] - probe_rate * red_other[p, q * n : (q + 1) * n] / tiles

    to_mate.wait_send()

    @pl.when(has_up)
    def _():
        to_up.wait_send()
        relay_up.wait_send()
        edge_up.wait_send()

    @pl.when(has_down)
    def _():
        to_down.wait_send()
        relay_down.wait_send()
        edge_down.wait_send()

    for p in range(modes // 2):

        def drain(hop):
            to, copy = scatter(p, hop)
            pl.when(to < owners)(copy.wait_send)
            pl.when(me < owners)(gather(p, hop).wait_send)

        each_peer(rows, drain)


def body(rows, object_field, probe, patterns, offsets, counts):
    modes, _, n, _ = probe.shape
    slots = patterns.shape[2]
    pairs = modes // 2
    owners = min(rows, 2 * n // 8)
    tables = jnp.asarray(dft_tables(n))
    vmem = pl.BlockSpec(memory_space=pltpu.VMEM)
    smem = pl.BlockSpec(memory_space=pltpu.SMEM)
    dma = pltpu.SemaphoreType.DMA
    wide, tall = (slots, 2 * n, modes * n), (slots, modes * n, 2 * n)
    return pl.pallas_call(
        functools.partial(kernel, rows, modes, slots, n, owners),
        out_shape=(
            jax.ShapeDtypeStruct(object_field.shape, F32),
            jax.ShapeDtypeStruct(probe.shape, F32),
        ),
        in_specs=[smem, smem, vmem, vmem, vmem, vmem],
        out_specs=(vmem, vmem),
        scratch_shapes=[
            pltpu.VMEM((3, 3, 2, n, n), F32),
            pltpu.VMEM(tall, BF16),
            pltpu.VMEM(tall, BF16),
            pltpu.VMEM(wide, BF16),
            pltpu.VMEM(wide, BF16),
            pltpu.VMEM(wide, F32),
            pltpu.VMEM((slots, 2 * n, 2 * n), BF16),
            pltpu.VMEM((slots, 2 * n, 2 * n), BF16),
            pltpu.VMEM((slots, 2, n, n), F32),
            pltpu.VMEM((slots, 2, n, n), F32),
            pltpu.VMEM((3, 2, n, n), F32),
            pltpu.VMEM((3, 2, n, n), F32),
            pltpu.VMEM((3, 2, n, n), F32),
            pltpu.VMEM((2, 2, n, n), F32),
            pltpu.VMEM((modes, 2, n, n), F32),
            pltpu.VMEM((pairs, 2, n, n), F32),
            pltpu.VMEM((pairs, 2 * n, n), F32),
            pltpu.VMEM((pairs, rows, 2 * n // owners, n), F32),
            pltpu.VMEM((pairs, 2 * n, n), F32),
            pltpu.VMEM((pairs, 2 * n, n), F32),
            dma((5,)), dma((5,)), dma((1,)), dma((1,)), dma((2,)), dma((2,)),
            dma((pairs,)), dma((pairs,)),
            dma((pairs, rows)), dma((pairs, rows)), dma((pairs, rows)), dma((pairs, rows)),
            dma((pairs,)), dma((pairs,)),
        ],
        compiler_params=pltpu.CompilerParams(collective_id=0, has_side_effects=True),
    )(offsets, counts, object_field, probe, patterns, tables)


def solution(mesh):
    placed = (
        P(None, ("tilt", "row"), "col"),
        P("tilt", None, None, None),
        P(("tilt", "row"), "col", None, None, None),
        P(("tilt", "row"), "col", None, None),
        P(("tilt", "row"), "col"),
    )
    return jax.shard_map(
        functools.partial(body, mesh.shape["row"]),
        mesh=mesh,
        in_specs=placed,
        out_specs=(P(None, ("tilt", "row"), "col"), P("tilt", None, None, None)),
        check_vma=False,
    )
```

```python
import functools

import jax
import jax.numpy as jnp
import numpy as np
from jax import lax
from jax.experimental import pallas as pl
from jax.experimental.pallas import tpu as pltpu
from jax.sharding import PartitionSpec as P

MESH = pl.DeviceIdType.MESH
F32 = jnp.float32
BF16 = jnp.bfloat16

object_rate = 1.0
probe_rate = 1.0
epsilon = 1e-06


def split_table(table):
    high = table.astype(jnp.bfloat16)
    low = (table - high.astype(np.float64)).astype(jnp.bfloat16)
    return high, low


def dft_tables(length):
    counter = np.arange(length)
    product = counter[:, None] * counter[None, :] % length
    angle = -2.0 * np.pi / length * product
    c, s = np.cos(angle) / np.sqrt(length), np.sin(angle) / np.sqrt(length)
    right = np.block([[c, s], [-s, c]])
    left = right.T
    return np.stack([*split_table(right), *split_table(left)])


def split(x):
    high = x.astype(BF16)
    return high, (x - high.astype(F32)).astype(BF16)


def each_peer(total, step):
    if total <= 16:
        for hop in range(1, total):
            step(hop)
    else:
        lax.fori_loop(1, total, lambda hop, carry: (step(hop), carry)[1], 0)


def dot(a, b):
    return jnp.dot(a, b, preferred_element_type=F32)


def kernel(
    rows, modes, slots, width, owners,
    off_ref, cnt_ref, obj_ref, probe_ref, pat_ref, tab_ref,
    obj_out, probe_out,
    frame, xh, xl, yh, yl, far, vh, vl, win, gacc,
    gown, gpar, grecv, gedge, term, tpart, acc, pieces, red, red_other,
    h_send, h_recv, g_send, g_recv, e_send, e_recv, t_send, t_recv,
    rs_send, rs_recv, ag_send, ag_recv, o_send, o_recv, news,
):
    me = lax.axis_index("row")
    col = lax.axis_index("col")
    n = width
    tiles = rows * 2
    mate = {"col": 1 - col}
    odd = lax.rem(me, 2)
    pair = {"row": me + 1 - 2 * odd}
    ahead, behind = me + 2 - 4 * odd, me - 2 + 4 * odd
    has_ahead = jnp.logical_and(ahead >= 0, ahead < rows)
    has_behind = jnp.logical_and(behind >= 0, behind < rows)
    chunk = 2 * n // owners

    def if_row(row, act):
        pl.when(jnp.logical_and(row >= 0, row < rows))(lambda: act({"row": row}))

    def present(distance):
        return (me >= distance).astype(jnp.int32) + (me + distance < rows).astype(jnp.int32)

    barrier = pltpu.get_barrier_semaphore()

    def greet(to):
        pl.semaphore_signal(barrier, inc=1, device_id=to, device_id_type=MESH)

    greet(mate)
    greet(pair)
    if_row(me - 2, greet)
    if_row(me + 2, greet)
    pl.semaphore_wait(barrier, 2 + present(2))

    rounds = [2]
    while 2 * rounds[-1] < rows:
        rounds.append(2 * rounds[-1])

    def tell(r):
        def act(to):
            pl.semaphore_signal(news.at[r], inc=1, device_id=to, device_id_type=MESH)

        if_row(me - rounds[r], act)
        if_row(me + rounds[r], act)

    def hear(r):
        pl.semaphore_wait(news.at[r], present(rounds[r]))

    def remote(src, dst, send, recv, to):
        return pltpu.make_async_remote_copy(
            src_ref=src, dst_ref=dst, send_sem=send, recv_sem=recv, device_id=to, device_id_type=MESH
        )

    seen = 2 * col
    mine = 2 - 2 * col
    pj, fj = 2 - 2 * odd, 2 * odd
    to_mate = remote(obj_ref, frame.at[1, seen], h_send.at[0], h_recv.at[0], mate)
    swaps, hops, relays, passes = [], [], [], []
    for q in range(2):
        swaps.append(remote(obj_ref.at[q], frame.at[fj, 1, q], h_send.at[1 + q], h_recv.at[1 + q], pair))
        hops.append(remote(frame.at[pj, 1, q], frame.at[fj, 1, q], h_send.at[3 + q], h_recv.at[3 + q], {"row": ahead}))
        relays.append(remote(frame.at[pj, 1, q], frame.at[pj, seen, q], h_send.at[5 + q], h_recv.at[5 + q], mate))
        passes.append(remote(frame.at[fj, 1, q], frame.at[fj, seen, q], h_send.at[7 + q], h_recv.at[7 + q], mate))
    for q in range(2):
        swaps[q].start()
    to_mate.start()
    tell(0)

    zero = jnp.zeros((2, n, n), F32)
    frame[1, 1] = obj_ref[...]
    for j in range(3):
        frame[j, seen] = zero

    @pl.when(jnp.logical_not(has_behind))
    def _():
        frame[fj, 1] = zero
        frame[fj, mine] = zero

    power = jnp.zeros((n, n), F32)
    for k in range(modes):
        power = power + (probe_ref[k, 0] * probe_ref[k, 0] + probe_ref[k, 1] * probe_ref[k, 1])
    weight = jnp.max(power) + epsilon

    for q in range(2):
        swaps[q].wait_recv()
        pl.when(has_ahead)(hops[q].start)
        relays[q].start()
    for q in range(2):

        @pl.when(has_behind)
        def _():
            hops[q].wait_recv()
            passes[q].start()

    to_mate.wait_recv()
    for q in range(2):
        relays[q].wait_recv()
        pl.when(has_behind)(passes[q].wait_recv)
    for r in range(len(rounds)):
        if r:
            tell(r)
        if r == 0 or r < len(rounds) - 1:
            hear(r)

    r_hi, r_lo, l_hi, l_lo = (tab_ref.at[t] for t in range(4))
    row_id = lax.broadcasted_iota(jnp.int32, (n, n), 0)
    lane_id = lax.broadcasted_iota(jnp.int32, (n, n), 1)

    def place(s):
        oy, ox = off_ref[0, 0, s, 0], off_ref[0, 0, s, 1]
        by, bx = oy // n, ox // n
        return by, bx, oy - by * n, ox - bx * n

    for s in range(slots):
        by, bx, sy, sx = place(s)
        by2, bx2 = jnp.minimum(by + 1, 2), jnp.minimum(bx + 1, 2)
        for q in range(2):
            upper = jnp.where(lane_id >= sx, frame[by, bx, q], frame[by, bx2, q])
            lower = jnp.where(lane_id >= sx, frame[by2, bx, q], frame[by2, bx2, q])
            packed = jnp.where(row_id >= sy, upper, lower)
            packed = pltpu.roll(packed, lax.rem(n - sy, n), 0)
            win[s, q] = pltpu.roll(packed, lax.rem(n - sx, n), 1)
        for k in range(modes):
            wr, wi = win[s, 0], win[s, 1]
            pr, pi = probe_ref[k, 0], probe_ref[k, 1]
            for q, part in enumerate((pr * wr - pi * wi, pr * wi + pi * wr)):
                hi, lo = split(part)
                xh[s, k * n : (k + 1) * n, q * n : (q + 1) * n] = hi
                xl[s, k * n : (k + 1) * n, q * n : (q + 1) * n] = lo
        for k in range(modes):
            a_hi, a_lo = xh[s, k * n : (k + 1) * n, :], xl[s, k * n : (k + 1) * n, :]
            y = dot(a_hi, r_hi[...]) + dot(a_lo, r_hi[...]) + dot(a_hi, r_lo[...])
            for q in range(2):
                hi, lo = split(y[:, q * n : (q + 1) * n])
                yh[s, q * n : (q + 1) * n, k * n : (k + 1) * n] = hi
                yl[s, q * n : (q + 1) * n, k * n : (k + 1) * n] = lo
        for p in range(modes // 2):
            cols = slice(2 * p * n, 2 * (p + 1) * n)
            b_hi, b_lo = yh[s, :, cols], yl[s, :, cols]
            far[s, :, cols] = dot(l_hi[...], b_hi) + dot(l_lo[...], b_hi) + dot(l_hi[...], b_lo)
        level = jnp.zeros((n, n), F32)
        for k in range(modes):
            cols = slice(k * n, (k + 1) * n)
            level = level + far[s, :n, cols] * far[s, :n, cols] + far[s, n:, cols] * far[s, n:, cols]
        live = (s < cnt_ref[0, 0]).astype(F32)
        misfit = live * (level - pat_ref[0, 0, s])
        for k in range(modes):
            for q in range(2):
                spot = (s, slice(q * n, (q + 1) * n), slice(k * n, (k + 1) * n))
                hi, lo = split(misfit * far[spot])
                yh[spot] = hi
                yl[spot] = lo

    def to_partner(p):
        return remote(term.at[2 * p + 1 - col], tpart.at[p], t_send.at[p], t_recv.at[p], mate)

    for p in range(modes // 2):
        cols = slice(2 * p * n, 2 * (p + 1) * n)
        for s in range(slots):
            b_hi, b_lo = yh[s, :, cols], yl[s, :, cols]
            v = dot(r_hi[...], b_hi) + dot(r_lo[...], b_hi) + dot(r_hi[...], b_lo)
            for m in range(2):
                for q in range(2):
                    hi, lo = split(v[q * n : (q + 1) * n, m * n : (m + 1) * n])
                    vh[s, m * n : (m + 1) * n, q * n : (q + 1) * n] = hi
                    vl[s, m * n : (m + 1) * n, q * n : (q + 1) * n] = lo
            for m in range(2):
                k = 2 * p + m
                a_hi, a_lo = vh[s, m * n : (m + 1) * n, :], vl[s, m * n : (m + 1) * n, :]
                back = dot(a_hi, l_hi[...]) + dot(a_lo, l_hi[...]) + dot(a_hi, l_lo[...])
                br, bi = back[:, :n], back[:, n:]
                pr, pi = probe_ref[k, 0], probe_ref[k, 1]
                gr, gi = pr * br + pi * bi, pr * bi - pi * br
                wr, wi = win[s, 0], win[s, 1]
                tr, ti = wr * br + wi * bi, wr * bi - wi * br
                if k == 0:
                    gacc[s, 0], gacc[s, 1] = gr, gi
                else:
                    gacc[s, 0], gacc[s, 1] = gacc[s, 0] + gr, gacc[s, 1] + gi
                if s == 0:
                    term[k, 0], term[k, 1] = tr, ti
                else:
                    term[k, 0], term[k, 1] = term[k, 0] + tr, term[k, 1] + ti
        to_partner(p).start()

    for q in range(2):
        own = [jnp.zeros((n, n), F32)] * 3
        par = [jnp.zeros((n, n), F32)] * 3
        for s in range(slots):
            by, bx, sy, sx = place(s)
            g = pltpu.roll(pltpu.roll(gacc[s, q], sy, 0), sx, 1)
            low_x, low_y = (lane_id >= sx).astype(F32), (row_id >= sy).astype(F32)

            def side(block, at, low):
                return (block == at).astype(F32) * low + (block == at + 1).astype(F32) * (1.0 - low)

            g_own, g_par = g * side(1, bx, low_x), g * side(mine, bx, low_x)
            for j in range(3):
                mask = side(j, by, low_y)
                own[j] = own[j] + g_own * mask
                par[j] = par[j] + g_par * mask
        for j in range(3):
            gown[j, q] = own[j]
            gpar[j, q] = par[j]
    across = remote(gpar, grecv, g_send.at[0], g_recv.at[0], mate)
    across.start()

    def row_slice(ref, p, owner):
        return ref.at[p, pl.ds(pl.multiple_of(owner * chunk, 8), chunk)]

    def scatter(p, hop):
        to = lax.rem(me + hop, rows)
        src = lax.rem(me + rows - hop, rows)
        return (
            to,
            remote(row_slice(acc, p, to), pieces.at[p, hop], rs_send.at[p, hop], rs_recv.at[p, hop], {"row": to}),
        )

    def start_scatter(p):
        to_partner(p).wait()
        for q in range(2):
            acc[p, q * n : (q + 1) * n] = term[2 * p + col, q] + tpart[p, q]

        def step(hop):
            to, copy = scatter(p, hop)
            pl.when(to < owners)(copy.start)

        each_peer(rows, step)

    if len(rounds) > 1:
        hear(len(rounds) - 1)
    start_scatter(0)

    across.wait()
    for j in range(3):
        gown[j] = gown[j] + grecv[j]
    edge_far = remote(gown.at[fj], gedge.at[0], e_send.at[0], e_recv.at[0], {"row": behind})
    edge_near = remote(gown.at[pj], gedge.at[1], e_send.at[1], e_recv.at[1], pair)
    pl.when(has_behind)(edge_far.start)

    for p in range(1, modes // 2):
        start_scatter(p)

    @pl.when(has_ahead)
    def _():
        edge_far.wait_recv()
        gown[pj] = gown[pj] + gedge[0]

    edge_near.start()

    def gather(p, hop):
        to = lax.rem(me + hop, rows)
        here = row_slice(red, p, me)
        return remote(here, here, ag_send.at[p, hop], ag_recv.at[p, hop], {"row": to})

    for p in range(modes // 2):

        @pl.when(me < owners)
        def _():
            red_chunk = row_slice(acc, p, me)[...]

            if rows <= 16:
                for hop in range(1, rows):
                    scatter(p, hop)[1].wait_recv()
                    red_chunk = red_chunk + pieces[p, hop]
            else:

                def add(hop, total):
                    scatter(p, hop)[1].wait_recv()
                    return total + pieces[p, hop]

                red_chunk = lax.fori_loop(1, rows, add, red_chunk)
            row_slice(red, p, me)[...] = red_chunk
            each_peer(rows, lambda hop: gather(p, hop).start())

    edge_near.wait_recv()
    for q in range(2):
        obj_out[q] = object_rate * (gown[1, q] + gedge[1, q]) / weight

    def swap(p):
        return remote(red.at[p], red_other.at[p], o_send.at[p], o_recv.at[p], mate)

    for p in range(modes // 2):

        def step(hop):
            src = lax.rem(me + rows - hop, rows)
            pl.when(src < owners)(gather(p, hop).wait_recv)

        each_peer(rows, step)
        swap(p).start()
        k = 2 * p + col
        for q in range(2):
            probe_out[k, q] = probe_rate * red[p, q * n : (q + 1) * n] / tiles
    for p in range(modes // 2):
        swap(p).wait()
        k = 2 * p + 1 - col
        for q in range(2):
            probe_out[k, q] = probe_rate * red_other[p, q * n : (q + 1) * n] / tiles

    to_mate.wait_send()
    edge_near.wait_send()
    pl.when(has_behind)(edge_far.wait_send)
    for q in range(2):
        swaps[q].wait_send()
        relays[q].wait_send()
        pl.when(has_ahead)(hops[q].wait_send)
        pl.when(has_behind)(passes[q].wait_send)

    for p in range(modes // 2):

        def drain(hop):
            to, copy = scatter(p, hop)
            pl.when(to < owners)(copy.wait_send)
            pl.when(me < owners)(gather(p, hop).wait_send)

        each_peer(rows, drain)


def finish(obj_ref, probe_ref, obj_step, probe_step, obj_out, probe_out):
    obj_out[...] = obj_ref[...] - obj_step[...]
    probe_out[...] = probe_ref[...] - probe_step[...]


def body(rows, object_field, probe, patterns, offsets, counts):
    modes, _, n, _ = probe.shape
    slots = patterns.shape[2]
    pairs = modes // 2
    owners = min(rows, 2 * n // 8)
    tables = jnp.asarray(dft_tables(n))
    vmem = pl.BlockSpec(memory_space=pltpu.VMEM)
    smem = pl.BlockSpec(memory_space=pltpu.SMEM)
    dma = pltpu.SemaphoreType.DMA
    wide, tall = (slots, 2 * n, modes * n), (slots, modes * n, 2 * n)
    steps = pl.pallas_call(
        functools.partial(kernel, rows, modes, slots, n, owners),
        out_shape=(
            jax.ShapeDtypeStruct(object_field.shape, F32),
            jax.ShapeDtypeStruct(probe.shape, F32),
        ),
        in_specs=[smem, smem, vmem, vmem, vmem, vmem],
        out_specs=(vmem, vmem),
        scratch_shapes=[
            pltpu.VMEM((3, 3, 2, n, n), F32),
            pltpu.VMEM(tall, BF16),
            pltpu.VMEM(tall, BF16),
            pltpu.VMEM(wide, BF16),
            pltpu.VMEM(wide, BF16),
            pltpu.VMEM(wide, F32),
            pltpu.VMEM((slots, 2 * n, 2 * n), BF16),
            pltpu.VMEM((slots, 2 * n, 2 * n), BF16),
            pltpu.VMEM((slots, 2, n, n), F32),
            pltpu.VMEM((slots, 2, n, n), F32),
            pltpu.VMEM((3, 2, n, n), F32),
            pltpu.VMEM((3, 2, n, n), F32),
            pltpu.VMEM((3, 2, n, n), F32),
            pltpu.VMEM((2, 2, n, n), F32),
            pltpu.VMEM((modes, 2, n, n), F32),
            pltpu.VMEM((pairs, 2, n, n), F32),
            pltpu.VMEM((pairs, 2 * n, n), F32),
            pltpu.VMEM((pairs, rows, 2 * n // owners, n), F32),
            pltpu.VMEM((pairs, 2 * n, n), F32),
            pltpu.VMEM((pairs, 2 * n, n), F32),
            dma((9,)), dma((9,)), dma((1,)), dma((1,)), dma((2,)), dma((2,)),
            dma((pairs,)), dma((pairs,)),
            dma((pairs, rows)), dma((pairs, rows)), dma((pairs, rows)), dma((pairs, rows)),
            dma((pairs,)), dma((pairs,)), pltpu.SemaphoreType.REGULAR((max(1, rows.bit_length()),)),
        ],
        compiler_params=pltpu.CompilerParams(collective_id=0, has_side_effects=True),
    )(offsets, counts, object_field, probe, patterns, tables)
    return pl.pallas_call(
        finish,
        out_shape=(
            jax.ShapeDtypeStruct(object_field.shape, F32),
            jax.ShapeDtypeStruct(probe.shape, F32),
        ),
        in_specs=[vmem] * 4,
        out_specs=(vmem, vmem),
    )(object_field, probe, *steps)


def solution(mesh):
    placed = (
        P(None, ("tilt", "row"), "col"),
        P("tilt", None, None, None),
        P(("tilt", "row"), "col", None, None, None),
        P(("tilt", "row"), "col", None, None),
        P(("tilt", "row"), "col"),
    )
    return jax.shard_map(
        functools.partial(body, mesh.shape["row"]),
        mesh=mesh,
        in_specs=placed,
        out_specs=(P(None, ("tilt", "row"), "col"), P("tilt", None, None, None)),
        check_vma=False,
    )
```

```python
import functools

import jax
import jax.numpy as jnp
import numpy as np
from jax import lax
from jax.experimental import pallas as pl
from jax.experimental.pallas import tpu as pltpu
from jax.sharding import PartitionSpec as P

MESH = pl.DeviceIdType.MESH
F32 = jnp.float32
BF16 = jnp.bfloat16

object_rate = 1.0
probe_rate = 1.0
epsilon = 1e-06


def split_table(table):
    high = table.astype(jnp.bfloat16)
    low = (table - high.astype(np.float64)).astype(jnp.bfloat16)
    return high, low


def dft_tables(length):
    counter = np.arange(length)
    product = counter[:, None] * counter[None, :] % length
    angle = -2.0 * np.pi / length * product
    c, s = np.cos(angle) / np.sqrt(length), np.sin(angle) / np.sqrt(length)
    right = np.block([[c, s], [-s, c]])
    left = right.T
    return np.stack([*split_table(right), *split_table(left)])


def split(x):
    high = x.astype(BF16)
    return high, (x - high.astype(F32)).astype(BF16)


def each_peer(total, step):
    if total <= 16:
        for hop in range(1, total):
            step(hop)
    else:
        lax.fori_loop(1, total, lambda hop, carry: (step(hop), carry)[1], 0)


def dot(a, b):
    return jnp.dot(a, b, preferred_element_type=F32)


def kernel(
    rows, modes, slots, width, owners,
    off_ref, cnt_ref, obj_ref, probe_ref, pat_ref, tab_ref,
    obj_out, probe_out,
    frame, xh, xl, yh, yl, far, vh, vl, win, gacc,
    gown, gpar, grecv, gedge, term, tpart, acc, pieces, red, red_other,
    h_send, h_recv, g_send, g_recv, e_send, e_recv, t_send, t_recv,
    rs_send, rs_recv, ag_send, ag_recv, o_send, o_recv, news,
):
    me = lax.axis_index("row")
    col = lax.axis_index("col")
    n = width
    tiles = rows * 2
    mate = {"col": 1 - col}
    up = {"row": me - 1}
    down = {"row": me + 1}
    has_up, has_down = me > 0, me < rows - 1
    chunk = 2 * n // owners

    def if_row(row, act):
        pl.when(jnp.logical_and(row >= 0, row < rows))(lambda: act({"row": row}))

    def present(distance):
        return (me >= distance).astype(jnp.int32) + (me + distance < rows).astype(jnp.int32)

    barrier = pltpu.get_barrier_semaphore()

    def greet(to):
        pl.semaphore_signal(barrier, inc=1, device_id=to, device_id_type=MESH)

    if_row(me + 1, greet)
    if_row(me - 1, greet)
    greet(mate)
    pl.semaphore_wait(barrier, 1 + present(1))

    rounds = [2]
    while 2 * rounds[-1] < rows:
        rounds.append(2 * rounds[-1])

    def tell(r):
        def act(to):
            pl.semaphore_signal(news.at[r], inc=1, device_id=to, device_id_type=MESH)

        if_row(me - rounds[r], act)
        if_row(me + rounds[r], act)

    def hear(r):
        pl.semaphore_wait(news.at[r], present(rounds[r]))

    def remote(src, dst, send, recv, to):
        return pltpu.make_async_remote_copy(
            src_ref=src, dst_ref=dst, send_sem=send, recv_sem=recv, device_id=to, device_id_type=MESH
        )

    seen = 2 * col
    mine = 2 - 2 * col
    to_mate = remote(obj_ref, frame.at[1, seen], h_send.at[0], h_recv.at[0], mate)
    to_up = remote(obj_ref, frame.at[2, 1], h_send.at[1], h_recv.at[2], up)
    to_down = remote(obj_ref, frame.at[0, 1], h_send.at[2], h_recv.at[1], down)
    relay_up = remote(frame.at[0, 1], frame.at[0, seen], h_send.at[3], h_recv.at[3], mate)
    relay_down = remote(frame.at[2, 1], frame.at[2, seen], h_send.at[4], h_recv.at[4], mate)
    pl.when(has_up)(to_up.start)
    pl.when(has_down)(to_down.start)
    to_mate.start()

    zero = jnp.zeros((2, n, n), F32)
    frame[1, 1] = obj_ref[...]
    for j in range(3):
        frame[j, seen] = zero

    @pl.when(me == 0)
    def _():
        frame[0, 1] = zero
        frame[0, mine] = zero

    @pl.when(me == rows - 1)
    def _():
        frame[2, 1] = zero
        frame[2, mine] = zero

    power = jnp.zeros((n, n), F32)
    for k in range(modes):
        power = power + (probe_ref[k, 0] * probe_ref[k, 0] + probe_ref[k, 1] * probe_ref[k, 1])
    weight = jnp.max(power) + epsilon

    @pl.when(has_up)
    def _():
        to_down.wait_recv()
        relay_up.start()

    @pl.when(has_down)
    def _():
        to_up.wait_recv()
        relay_down.start()

    to_mate.wait_recv()
    pl.when(has_up)(relay_up.wait_recv)
    pl.when(has_down)(relay_down.wait_recv)

    tell(0)

    r_hi, r_lo, l_hi, l_lo = (tab_ref.at[t] for t in range(4))
    row_id = lax.broadcasted_iota(jnp.int32, (n, n), 0)
    lane_id = lax.broadcasted_iota(jnp.int32, (n, n), 1)

    def place(s):
        oy, ox = off_ref[0, 0, s, 0], off_ref[0, 0, s, 1]
        by, bx = oy // n, ox // n
        return by, bx, oy - by * n, ox - bx * n

    for s in range(slots):
        by, bx, sy, sx = place(s)
        by2, bx2 = jnp.minimum(by + 1, 2), jnp.minimum(bx + 1, 2)
        for q in range(2):
            upper = jnp.where(lane_id >= sx, frame[by, bx, q], frame[by, bx2, q])
            lower = jnp.where(lane_id >= sx, frame[by2, bx, q], frame[by2, bx2, q])
            packed = jnp.where(row_id >= sy, upper, lower)
            packed = pltpu.roll(packed, lax.rem(n - sy, n), 0)
            win[s, q] = pltpu.roll(packed, lax.rem(n - sx, n), 1)
        for k in range(modes):
            wr, wi = win[s, 0], win[s, 1]
            pr, pi = probe_ref[k, 0], probe_ref[k, 1]
            for q, part in enumerate((pr * wr - pi * wi, pr * wi + pi * wr)):
                hi, lo = split(part)
                xh[s, k * n : (k + 1) * n, q * n : (q + 1) * n] = hi
                xl[s, k * n : (k + 1) * n, q * n : (q + 1) * n] = lo
        for k in range(modes):
            a_hi, a_lo = xh[s, k * n : (k + 1) * n, :], xl[s, k * n : (k + 1) * n, :]
            y = dot(a_hi, r_hi[...]) + dot(a_lo, r_hi[...]) + dot(a_hi, r_lo[...])
            for q in range(2):
                hi, lo = split(y[:, q * n : (q + 1) * n])
                yh[s, q * n : (q + 1) * n, k * n : (k + 1) * n] = hi
                yl[s, q * n : (q + 1) * n, k * n : (k + 1) * n] = lo
        for p in range(modes // 2):
            cols = slice(2 * p * n, 2 * (p + 1) * n)
            b_hi, b_lo = yh[s, :, cols], yl[s, :, cols]
            far[s, :, cols] = dot(l_hi[...], b_hi) + dot(l_lo[...], b_hi) + dot(l_hi[...], b_lo)
        level = jnp.zeros((n, n), F32)
        for k in range(modes):
            cols = slice(k * n, (k + 1) * n)
            level = level + far[s, :n, cols] * far[s, :n, cols] + far[s, n:, cols] * far[s, n:, cols]
        live = (s < cnt_ref[0, 0]).astype(F32)
        misfit = live * (level - pat_ref[0, 0, s])
        for k in range(modes):
            for q in range(2):
                spot = (s, slice(q * n, (q + 1) * n), slice(k * n, (k + 1) * n))
                hi, lo = split(misfit * far[spot])
                yh[spot] = hi
                yl[spot] = lo

    for r in range(1, len(rounds)):
        hear(r - 1)
        tell(r)

    def to_partner(p):
        return remote(term.at[2 * p + 1 - col], tpart.at[p], t_send.at[p], t_recv.at[p], mate)

    for p in range(modes // 2):
        cols = slice(2 * p * n, 2 * (p + 1) * n)
        for s in range(slots):
            b_hi, b_lo = yh[s, :, cols], yl[s, :, cols]
            v = dot(r_hi[...], b_hi) + dot(r_lo[...], b_hi) + dot(r_hi[...], b_lo)
            for m in range(2):
                for q in range(2):
                    hi, lo = split(v[q * n : (q + 1) * n, m * n : (m + 1) * n])
                    vh[s, m * n : (m + 1) * n, q * n : (q + 1) * n] = hi
                    vl[s, m * n : (m + 1) * n, q * n : (q + 1) * n] = lo
            for m in range(2):
                k = 2 * p + m
                a_hi, a_lo = vh[s, m * n : (m + 1) * n, :], vl[s, m * n : (m + 1) * n, :]
                back = dot(a_hi, l_hi[...]) + dot(a_lo, l_hi[...]) + dot(a_hi, l_lo[...])
                br, bi = back[:, :n], back[:, n:]
                pr, pi = probe_ref[k, 0], probe_ref[k, 1]
                gr, gi = pr * br + pi * bi, pr * bi - pi * br
                wr, wi = win[s, 0], win[s, 1]
                tr, ti = wr * br + wi * bi, wr * bi - wi * br
                if k == 0:
                    gacc[s, 0], gacc[s, 1] = gr, gi
                else:
                    gacc[s, 0], gacc[s, 1] = gacc[s, 0] + gr, gacc[s, 1] + gi
                if s == 0:
                    term[k, 0], term[k, 1] = tr, ti
                else:
                    term[k, 0], term[k, 1] = term[k, 0] + tr, term[k, 1] + ti
        to_partner(p).start()

    def row_slice(ref, p, owner):
        return ref.at[p, pl.ds(pl.multiple_of(owner * chunk, 8), chunk)]

    def scatter(p, hop):
        to = lax.rem(me + hop, rows)
        src = lax.rem(me + rows - hop, rows)
        return (
            to,
            remote(row_slice(acc, p, to), pieces.at[p, hop], rs_send.at[p, hop], rs_recv.at[p, hop], {"row": to}),
        )

    def start_scatter(p):
        to_partner(p).wait()
        for q in range(2):
            acc[p, q * n : (q + 1) * n] = term[2 * p + col, q] + tpart[p, q]

        def step(hop):
            to, copy = scatter(p, hop)
            pl.when(to < owners)(copy.start)

        each_peer(rows, step)

    hear(len(rounds) - 1)
    start_scatter(0)

    for q in range(2):
        own = [jnp.zeros((n, n), F32)] * 3
        par = [jnp.zeros((n, n), F32)] * 3
        for s in range(slots):
            by, bx, sy, sx = place(s)
            g = pltpu.roll(pltpu.roll(gacc[s, q], sy, 0), sx, 1)
            low_x, low_y = (lane_id >= sx).astype(F32), (row_id >= sy).astype(F32)

            def side(block, at, low):
                return (block == at).astype(F32) * low + (block == at + 1).astype(F32) * (1.0 - low)

            g_own, g_par = g * side(1, bx, low_x), g * side(mine, bx, low_x)
            for j in range(3):
                mask = side(j, by, low_y)
                own[j] = own[j] + g_own * mask
                par[j] = par[j] + g_par * mask
        for j in range(3):
            gown[j, q] = own[j]
            gpar[j, q] = par[j]
    across = remote(gpar, grecv, g_send.at[0], g_recv.at[0], mate)
    across.start()


    for p in range(1, modes // 2):
        start_scatter(p)

    across.wait()
    for j in range(3):
        gown[j] = gown[j] + grecv[j]
    edge_up = remote(gown.at[0], gedge.at[1], e_send.at[0], e_recv.at[1], up)
    edge_down = remote(gown.at[2], gedge.at[0], e_send.at[1], e_recv.at[0], down)
    pl.when(has_up)(edge_up.start)
    pl.when(has_down)(edge_down.start)

    def gather(p, hop):
        to = lax.rem(me + hop, rows)
        here = row_slice(red, p, me)
        return remote(here, here, ag_send.at[p, hop], ag_recv.at[p, hop], {"row": to})

    for p in range(modes // 2):

        @pl.when(me < owners)
        def _():
            red_chunk = row_slice(acc, p, me)[...]

            if rows <= 16:
                for hop in range(1, rows):
                    scatter(p, hop)[1].wait_recv()
                    red_chunk = red_chunk + pieces[p, hop]
            else:

                def add(hop, total):
                    scatter(p, hop)[1].wait_recv()
                    return total + pieces[p, hop]

                red_chunk = lax.fori_loop(1, rows, add, red_chunk)
            row_slice(red, p, me)[...] = red_chunk
            each_peer(rows, lambda hop: gather(p, hop).start())

    @pl.when(jnp.logical_not(has_up))
    def _():
        gedge[0] = zero

    @pl.when(jnp.logical_not(has_down))
    def _():
        gedge[1] = zero

    pl.when(has_up)(edge_down.wait_recv)
    pl.when(has_down)(edge_up.wait_recv)
    for q in range(2):
        grad = gown[1, q] + gedge[0, q] + gedge[1, q]
        obj_out[q] = object_rate * grad / weight

    def swap(p):
        return remote(red.at[p], red_other.at[p], o_send.at[p], o_recv.at[p], mate)

    for p in range(modes // 2):

        def step(hop):
            src = lax.rem(me + rows - hop, rows)
            pl.when(src < owners)(gather(p, hop).wait_recv)

        each_peer(rows, step)
        swap(p).start()
        k = 2 * p + col
        for q in range(2):
            probe_out[k, q] = probe_rate * red[p, q * n : (q + 1) * n] / tiles
    for p in range(modes // 2):
        swap(p).wait()
        k = 2 * p + 1 - col
        for q in range(2):
            probe_out[k, q] = probe_rate * red_other[p, q * n : (q + 1) * n] / tiles

    to_mate.wait_send()

    @pl.when(has_up)
    def _():
        to_up.wait_send()
        relay_up.wait_send()
        edge_up.wait_send()

    @pl.when(has_down)
    def _():
        to_down.wait_send()
        relay_down.wait_send()
        edge_down.wait_send()

    for p in range(modes // 2):

        def drain(hop):
            to, copy = scatter(p, hop)
            pl.when(to < owners)(copy.wait_send)
            pl.when(me < owners)(gather(p, hop).wait_send)

        each_peer(rows, drain)


def finish(obj_ref, probe_ref, obj_step, probe_step, obj_out, probe_out):
    obj_out[...] = obj_ref[...] - obj_step[...]
    probe_out[...] = probe_ref[...] - probe_step[...]


def body(rows, object_field, probe, patterns, offsets, counts):
    modes, _, n, _ = probe.shape
    slots = patterns.shape[2]
    pairs = modes // 2
    owners = min(rows, 2 * n // 8)
    tables = jnp.asarray(dft_tables(n))
    vmem = pl.BlockSpec(memory_space=pltpu.VMEM)
    smem = pl.BlockSpec(memory_space=pltpu.SMEM)
    dma = pltpu.SemaphoreType.DMA
    wide, tall = (slots, 2 * n, modes * n), (slots, modes * n, 2 * n)
    steps = pl.pallas_call(
        functools.partial(kernel, rows, modes, slots, n, owners),
        out_shape=(
            jax.ShapeDtypeStruct(object_field.shape, F32),
            jax.ShapeDtypeStruct(probe.shape, F32),
        ),
        in_specs=[smem, smem, vmem, vmem, vmem, vmem],
        out_specs=(vmem, vmem),
        scratch_shapes=[
            pltpu.VMEM((3, 3, 2, n, n), F32),
            pltpu.VMEM(tall, BF16),
            pltpu.VMEM(tall, BF16),
            pltpu.VMEM(wide, BF16),
            pltpu.VMEM(wide, BF16),
            pltpu.VMEM(wide, F32),
            pltpu.VMEM((slots, 2 * n, 2 * n), BF16),
            pltpu.VMEM((slots, 2 * n, 2 * n), BF16),
            pltpu.VMEM((slots, 2, n, n), F32),
            pltpu.VMEM((slots, 2, n, n), F32),
            pltpu.VMEM((3, 2, n, n), F32),
            pltpu.VMEM((3, 2, n, n), F32),
            pltpu.VMEM((3, 2, n, n), F32),
            pltpu.VMEM((2, 2, n, n), F32),
            pltpu.VMEM((modes, 2, n, n), F32),
            pltpu.VMEM((pairs, 2, n, n), F32),
            pltpu.VMEM((pairs, 2 * n, n), F32),
            pltpu.VMEM((pairs, rows, 2 * n // owners, n), F32),
            pltpu.VMEM((pairs, 2 * n, n), F32),
            pltpu.VMEM((pairs, 2 * n, n), F32),
            dma((5,)), dma((5,)), dma((1,)), dma((1,)), dma((2,)), dma((2,)),
            dma((pairs,)), dma((pairs,)),
            dma((pairs, rows)), dma((pairs, rows)), dma((pairs, rows)), dma((pairs, rows)),
            dma((pairs,)), dma((pairs,)), pltpu.SemaphoreType.REGULAR((max(1, rows.bit_length()),)),
        ],
        compiler_params=pltpu.CompilerParams(collective_id=0, has_side_effects=True),
    )(offsets, counts, object_field, probe, patterns, tables)
    return pl.pallas_call(
        finish,
        out_shape=(
            jax.ShapeDtypeStruct(object_field.shape, F32),
            jax.ShapeDtypeStruct(probe.shape, F32),
        ),
        in_specs=[vmem] * 4,
        out_specs=(vmem, vmem),
    )(object_field, probe, *steps)


def solution(mesh):
    placed = (
        P(None, ("tilt", "row"), "col"),
        P("tilt", None, None, None),
        P(("tilt", "row"), "col", None, None, None),
        P(("tilt", "row"), "col", None, None),
        P(("tilt", "row"), "col"),
    )
    return jax.shard_map(
        functools.partial(body, mesh.shape["row"]),
        mesh=mesh,
        in_specs=placed,
        out_specs=(P(None, ("tilt", "row"), "col"), P("tilt", None, None, None)),
        check_vma=False,
    )
```
